32 devices in a mesh: gx: 8 (over z, y), gy: 4 (over x, core).
Axes of the slice: x: 2, y: 2, z: 4, core: 2. Of those that a mesh axis runs over, the one named last changes fastest.
Arguments:
- hidden: bfloat16 [4096, 14336], P('gx', 'gy'), may hold values from -6 to 6
- weight: bfloat16 [4096, 14336], P(None, 'gy'), may hold values from -0.0625 to 0.0625
- cotangent: bfloat16 [4096, 4096], P('gx', 'gy'), may hold values from -6 to 6
Outputs:
- output: bfloat16 [4096, 4096], P('gx', 'gy')
- hidden_grad: bfloat16 [4096, 14336], P('gx', 'gy')
- weight_grad: float32 [4096, 14336], P('gx', 'gy')
The draws below stay inside these ranges and needn't reach their ends.
All inputs are finite; a program needn't handle non-finite values.
Results may differ from the reference program's by a relative error of at most 0.001.
Values may be sent and summed in bfloat16 or wider, within the bound.
A program may use at most 128 MiB of HBM per device.

```python
import jax
import jax.numpy as jnp

D = 4096
FF = 14336
TOKENS = 4096


def strengthened(values, rng, source, target, blocks, factor):
    def block_of(position):
        return (jnp.arange(values.shape[position]) // (values.shape[position] // blocks)).reshape((-1,) + (1,) * (values.ndim - 1 - position))

    near = jax.random.permutation(rng, blocks)[block_of(target)]
    far = (block_of(target) + blocks // 2) % blocks
    return jnp.where((block_of(source) == near) | (block_of(source) == far), factor * values, values)


def block_scale(rng, dims, pieces, smallest, high):
    gain, own = 1.0, jax.random.fold_in(rng, 6)
    for position, blocks in pieces:
        heights = jnp.exp(jax.random.uniform(jax.random.fold_in(own, position), (blocks,), jnp.float32, smallest / len(pieces), high / len(pieces)))
        gain = gain * jnp.repeat(heights, dims[position] // blocks).reshape([-1 if axis == position else 1 for axis in range(len(dims))])
    return gain


def scatter_about(own_key, dims, spread, limit, shards=(), held_as=jnp.bfloat16):
    loudness = block_scale(own_key, dims, shards, -0.22, 0.18) if shards else 1.0
    values = jax.random.normal(own_key, dims, jnp.float32) * spread * loudness
    return jnp.minimum(jnp.maximum(values, -limit), limit).astype(held_as)


def gaussian_with(stream_key, shape, deviation, reach, split, heavy, kind=jnp.bfloat16):
    result = deviation * jax.random.normal(stream_key, shape, jnp.float32)
    if split:
        result = result * block_scale(stream_key, shape, split, -0.22, 0.18)
    return jnp.clip(strengthened(result, jax.random.fold_in(stream_key, 3), *heavy), -reach, reach).astype(kind)


def setup_inputs(seed: int = 0) -> dict:
    arg_keys = jax.random.split(jax.random.key(seed), 4)
    hidden = scatter_about(arg_keys[0], (TOKENS, FF), 1.0, 6.0, ((0, 8), (1, 4)))
    weight = gaussian_with(arg_keys[1], (D, FF), FF ** -0.5, 0.0625, ((1, 4),), (1, 0, 4, 2.0))
    cotangent = gaussian_with(arg_keys[2], (TOKENS, D), 1.0, 6.0, ((0, 8), (1, 4)), (0, 1, 8, 2.0))
    return {"hidden": hidden, "weight": weight, "cotangent": cotangent}


def reference(hidden, weight, cotangent):
    hidden_f = hidden.astype(jnp.float32)
    weight_f = weight.astype(jnp.float32)
    cotangent_f = cotangent.astype(jnp.float32)
    output = jnp.dot(hidden_f, weight_f.T, preferred_element_type=jnp.float32).astype(jnp.bfloat16)
    hidden_grad = jnp.dot(cotangent_f, weight_f, preferred_element_type=jnp.float32).astype(jnp.bfloat16)
    weight_grad = jnp.dot(cotangent_f.T, hidden_f, preferred_element_type=jnp.float32) * (TOKENS ** -0.5)
    return output, hidden_grad, weight_grad
```

```python
import functools

import jax
import jax.numpy as jnp
from jax import lax
from jax.experimental import pallas as pl
from jax.experimental.pallas import tpu as pltpu
from jax.sharding import PartitionSpec as P


PAIR = 2
STREAMS = 4
LANES = 128


def cuts(width, pieces):
    units = width // LANES if width % LANES == 0 else width
    step = width // units
    pieces = min(pieces, units)
    edges = [units * i // pieces * step for i in range(pieces + 1)]
    return list(zip(edges[:-1], edges[1:]))


def dot_t(a, b):
    return lax.dot_general(a, b, (((0,), (0,)), ((), ())), preferred_element_type=jnp.float32)


def shards_ring(hidden, weight, cotangent):
    gx, gy = lax.axis_size("gx"), lax.axis_size("gy")
    nz, nx = gx // PAIR, gy // PAIR
    ix, iy = lax.axis_index("gx"), lax.axis_index("gy")
    z, y = ix // PAIR, ix % PAIR
    x, core = iy // PAIR, iy % PAIR
    rows, width = hidden.shape
    block = cotangent.shape[1]
    features = weight.shape[0]
    grad_scale = float(rows * gx) ** (-0.5)
    f32 = jnp.float32

    def z_shift(v, d):
        return lax.ppermute(v, "gx", [(g, (g + PAIR * d) % gx) for g in range(gx)])

    def y_swap(v):
        return lax.ppermute(v, "gx", [(g, g ^ 1) for g in range(gx)])

    def x_shift(v, d):
        return lax.ppermute(v, "gy", [(j, (j + PAIR * d) % gy) for j in range(gy)])

    def core_swap(v):
        return lax.ppermute(v, "gy", [(j, j ^ 1) for j in range(gy)])

    mine = jnp.stack([cotangent] + [x_shift(cotangent, d) for d in range(1, nx)])
    theirs = core_swap(mine)
    full = jnp.zeros((rows, features), cotangent.dtype)
    for d in range(nx):
        source = (x - d) % nx * PAIR
        full = lax.dynamic_update_slice(full, mine[d], (0, (source + core) * block))
        full = lax.dynamic_update_slice(full, theirs[d], (0, (source + 1 - core) * block))

    span = features // nz
    half = rows // PAIR
    fetched = jnp.stack(
        [
            z_shift(
                lax.dynamic_slice(full, (core * half, (z + t) % nz * span), (half, span)), t
            )
            for t in range(1, nz)
        ]
    )
    other = core_swap(fetched)
    low = jnp.where(core == 0, fetched, other)
    high = jnp.where(core == 0, other, fetched)
    by_shift = [lax.dynamic_slice(full, (0, z * span), (rows, span))]
    by_shift += [jnp.concatenate([low[t], high[t]]) for t in range(nz - 1)]
    rows_out = span // PAIR

    def of_feature_block(stack, which):
        return lax.dynamic_slice(stack, (0, which * rows_out), (rows * nz, rows_out))

    stacks = (
        jnp.concatenate(by_shift),
        jnp.concatenate([by_shift[-t % nz] for t in range(nz)]),
    )
    own = [of_feature_block(s, y) for s in stacks]
    peer = [of_feature_block(s, 1 - y) for s in stacks]

    partial = lax.dot_general(
        hidden, weight, (((1,), (1,)), ((), ())), preferred_element_type=f32
    )

    def columns(which_core):
        return jnp.stack(
            [
                lax.dynamic_slice(
                    partial, (0, ((x + d) % nx * PAIR + which_core) * block), (rows, block)
                )
                for d in range(nx)
            ]
        )

    chip_sum = columns(core) + core_swap(columns(1 - core))
    total = chip_sum[0]
    for d in range(1, nx):
        total = total + x_shift(chip_sum[d], d)
    output = total.astype(jnp.bfloat16)

    hidden_grad = jnp.dot(full, weight, preferred_element_type=f32).astype(jnp.bfloat16)

    weight_grad = jnp.zeros((rows_out, width), f32)
    for s, (start, stop) in enumerate(cuts(width, STREAMS)):
        way = 1 if s % 2 == 0 else -1
        held = [hidden[:, start:stop]]
        for _ in range(nz - 1):
            held.append(z_shift(held[-1], way))
        tokens = jnp.concatenate(held)
        arrived = y_swap(dot_t(peer[s % 2], tokens))
        summed = dot_t(own[s % 2], tokens) + arrived
        weight_grad = lax.dynamic_update_slice(weight_grad, summed * grad_scale, (0, start))
    return (output, hidden_grad, weight_grad)


MESH = pl.DeviceIdType.MESH
CHUNK = 2 * LANES
AHEAD = 2
Y_LAG = 2
Z_LAG = 4
HG_LAG = 3
SLOTS = 4
TOP = 2.0 ** 25


def encode(value, inverse_step):
    u = value * inverse_step
    square = u * u
    return (square * square * u).astype(jnp.bfloat16)


def decode(code, step):
    code = code.astype(jnp.float32)
    root = jnp.exp2(jnp.log2(jnp.maximum(jnp.abs(code), 1e-37)) * 0.2) * step
    return jnp.where(code > 0, root, jnp.where(code < 0, -root, 0.0))


def mirror_kernel(
    grad_scale, hidden, weight, cot, out, hgrad, wgrad,
    hid, tok, cotf, cotp, cot_peer, cot_own, wtile, wcols, part, crecv, xrecv,
    ysend, yrecv, msend, mrecv, wstage, hstage, ostage, maxima, arrived, scales,
    load_sem, tok_sem, wt_sem, wc_sem, c_send, c_recv, x_send, x_recv,
    t_send, t_recv, y_send, y_recv, m_send, m_recv, b_send, b_recv, ws_sem, hs_sem,
):
    f32 = jnp.float32
    ix, iy = lax.axis_index("gx"), lax.axis_index("gy")
    z, y = ix // 2, ix % 2
    x, core = iy // 2, iy % 2
    rows, width = hid.shape
    block = cotf.shape[1] // 4
    half = block // 2
    n = width // CHUNK
    per_block = block // CHUNK
    n_out = 4 * per_block

    to_core = (ix, x * 2 + 1 - core)
    to_x = (ix, (1 - x) * 2 + core)
    to_y = (z * 2 + 1 - y, iy)
    pair = z + 1 - 2 * (z % 2)
    mirror = 3 - z
    to_pair = (pair * 2 + y, iy)
    to_mirror = (mirror * 2 + y, iy)
    chosen = jnp.logical_or(iy == z, iy == 3 - z)
    x_block = (1 - x) * 2 + core

    def remote(src, dst, send, recv, device):
        return pltpu.make_async_remote_copy(
            src_ref=src, dst_ref=dst, send_sem=send, recv_sem=recv,
            device_id=device, device_id_type=MESH,
        )

    def at_block(j):
        return cotf.at[:, pl.ds(pl.multiple_of(j * block, block), block)]

    def cols(ref, s):
        return ref.at[:, pl.ds(pl.multiple_of(s * CHUNK, CHUNK), CHUNK)]

    first = jnp.where(jnp.where(chosen, iy, x_block) == z, 0, 1)
    peer_slot = 1 - jnp.where(iy == z, 1, 0)
    core_own = remote(cot, at_block(iy), c_send.at[0], c_recv.at[0], to_core)
    x_own = remote(cot, at_block(iy), x_send.at[0], x_recv.at[0], to_x)
    relay_slot = jnp.where(iy == pair, 0, 1)
    z_cot = remote(cot, cotp.at[relay_slot], x_send.at[1], x_recv.at[1], to_pair)
    x_peer = remote(cotp.at[peer_slot], cotp.at[peer_slot], x_send.at[2], x_recv.at[2], to_x)
    core_relay = remote(at_block(x_block), at_block(x_block), c_send.at[1], c_recv.at[1], to_core)
    core_peer = remote(cotp.at[first], cotp.at[first], c_send.at[2], c_recv.at[2], to_core)
    core_part = [
        remote(part.at[2 * i], crecv.at[i], c_send.at[3 + i], c_recv.at[3 + i], to_core)
        for i in range(2)
    ]
    x_part = remote(part.at[1], xrecv, x_send.at[3], x_recv.at[3], to_x)

    def send_tokens(s):
        return remote(
            cols(hidden, s), tok.at[s, pl.ds(rows, rows)], t_send.at[s], t_recv.at[s], to_pair
        )

    def load_tokens(s):
        return pltpu.make_async_copy(cols(hidden, s), tok.at[s, pl.ds(0, rows)], tok_sem.at[s])

    def send_y(s):
        return remote(ysend.at[s % SLOTS], yrecv.at[s], y_send.at[s], y_recv.at[s], to_y)

    def send_mirror(s):
        return remote(msend.at[s % SLOTS], mrecv.at[s], m_send.at[s], m_recv.at[s], to_mirror)

    def load_rows(t):
        q, sub = t // per_block, t % per_block
        b = jnp.where(
            q == 0, 3 - iy, jnp.where(q == 1, x_block, jnp.where(q == 2, x * 2 + 1 - core, iy))
        )
        at = pl.multiple_of(b * block + sub * CHUNK, CHUNK)
        return pltpu.make_async_copy(
            weight.at[pl.ds(at, CHUNK)], wtile.at[t % 2], wt_sem.at[t % 2]
        )

    def load_cols(t):
        return pltpu.make_async_copy(cols(weight, t), wcols.at[t % 2], wc_sem.at[t % 2])

    def store_hgrad(t):
        return pltpu.make_async_copy(hstage.at[t % 2], cols(hgrad, t), hs_sem.at[t % 2])

    def store_wgrad(s):
        return pltpu.make_async_copy(wstage.at[s % 2], cols(wgrad, s), ws_sem.at[s % 2])

    load_hidden = pltpu.make_async_copy(hidden, hid, load_sem.at[0])
    load_cot = pltpu.make_async_copy(cot, at_block(iy), load_sem.at[1])
    load_hidden.start()
    load_cot.start()
    load_rows(0).start()

    barrier = pltpu.get_barrier_semaphore()
    for device in (to_core, to_x, to_y, to_pair, to_mirror):
        pl.semaphore_signal(barrier, inc=1, device_id=device, device_id_type=MESH)
    pl.semaphore_wait(barrier, 5)

    @pl.when(chosen)
    def _():
        x_own.start()

    @pl.when(jnp.logical_not(chosen))
    def _():
        z_cot.start()

    core_own.start()

    @pl.loop(0, n)
    def _(s):
        load_tokens(s).start()

    load_hidden.wait()
    load_cot.wait()

    stages = (to_core, to_x, to_pair, to_mirror, to_y)

    def exchange(i):
        return remote(maxima.at[i], arrived.at[i], b_send.at[i], b_recv.at[i], stages[i])

    def settle(i):
        exchange(i).wait_recv()
        maxima[i + 1] = jnp.maximum(maxima[i], arrived[i])

    def highest(ref, start, count):
        def body(i, best):
            at = pl.multiple_of(start + i * CHUNK, CHUNK)
            v = jnp.abs(ref[:, pl.ds(at, CHUNK)].astype(f32))
            return jnp.maximum(best, jnp.max(v.reshape(rows // 8, 8, CHUNK), axis=0))

        best = lax.fori_loop(0, count, body, jnp.zeros((8, CHUNK), f32))
        return jnp.full((8, LANES), jnp.max(best), f32)

    @pl.loop(0, n_out)
    def _(t):
        q, sub = t // per_block, t % per_block

        @pl.when(t + 1 < n_out)
        def _():
            load_rows(t + 1).start()

        @pl.when(t == 1)
        def _():
            maxima[0, 0:8] = highest(hid, 0, n)
            maxima[0, 8:16] = highest(cotf, iy * block, per_block)

        for i in range(5):
            @pl.when(t == 2 + 3 * i)
            def _():
                exchange(i).start()

            if i < 4:
                @pl.when(t == 4 + 3 * i)
                def _():
                    settle(i)

        @pl.when(t == per_block + 1)
        def _():
            core_part[0].start()

        @pl.when(t == 6)
        def _():
            send_tokens(0).start()

        @pl.when(t == 9)
        def _():
            send_tokens(1).start()

        @pl.when(t == 2 * per_block + 1)
        def _():
            core_part[0].wait_recv()

            @pl.loop(0, per_block)
            def _(k):
                at = pl.ds(pl.multiple_of(k * CHUNK, CHUNK), CHUNK)
                part[1, :, at] = part[1, :, at] + crecv[0, :, at]

        @pl.when(t == 11)
        def _():
            @pl.when(chosen)
            def _():
                z_cot.wait_recv()
                x_peer.start()
                core_peer.start()

            @pl.when(jnp.logical_not(chosen))
            def _():
                x_own.wait_recv()
                core_relay.start()

        @pl.when(t == 3 * per_block + 1)
        def _():
            core_part[1].start()

        load_rows(t).wait()
        part[q, :, pl.ds(pl.multiple_of(sub * CHUNK, CHUNK), CHUNK)] = lax.dot_general(
            hid[...], wtile[t % 2], (((1,), (1,)), ((), ())), preferred_element_type=f32
        )

    settle(4)
    load_cols(0).start()

    core_own.wait_recv()

    @pl.when(chosen)
    def _():
        core_relay.wait_recv()

    def turn(ref, lane, row):
        for r in range(2):
            at = pl.ds(pl.multiple_of(lane(r, y), half), half)
            cot_own[r, :, row * rows:(row + 1) * rows] = ref(r)[:, at].T
            at = pl.ds(pl.multiple_of(lane(r, 1 - y), half), half)
            cot_peer[r, :, row * rows:(row + 1) * rows] = ref(r)[:, at].T

    turn(lambda r: cotf, lambda r, h: (z if r == 0 else 3 - z) * block + h * half, 0)

    @pl.when(jnp.logical_not(chosen))
    def _():
        x_peer.wait_recv()
        core_peer.start()

    core_peer.wait_recv()

    @pl.when(jnp.logical_not(chosen))
    def _():
        x_own.start()

    turn(lambda r: cotp.at[r], lambda r, h: h * half, 1)

    best = maxima[5]
    step = jnp.maximum(best[0:8] * best[8:16] * (4.0 * rows / TOP), 1e-36)
    scales[0] = step
    scales[1] = 1.0 / step

    @pl.loop(0, n + Z_LAG)
    def _(s):
        @pl.when(s + AHEAD < n)
        def _():
            send_tokens(s + AHEAD).start()

        @pl.when(s < n)
        def _():
            load_tokens(s).wait()
            send_tokens(s).wait_recv()

            @pl.when(s >= SLOTS)
            def _():
                send_y(s - SLOTS).wait_send()

            inverse = scales[1, 0:1, 0:1]
            for r in range(2):
                ysend[s % SLOTS, r] = encode(
                    jnp.dot(cot_peer[r], tok[s], preferred_element_type=f32), inverse
                )

        @pl.when(s == 1)
        def _():
            x_part.start()

        @pl.when(s == HG_LAG)
        def _():
            @pl.when(chosen)
            def _():
                x_own.wait_recv()
                core_relay.start()

            @pl.when(jnp.logical_not(chosen))
            def _():
                core_relay.wait_recv()

        @pl.when(jnp.logical_and(s >= HG_LAG, s < n + HG_LAG))
        def _():
            t = s - HG_LAG

            @pl.when(t + 1 < n)
            def _():
                load_cols(t + 1).start()

            load_cols(t).wait()

            @pl.when(t >= 2)
            def _():
                store_hgrad(t - 2).wait()

            hstage[t % 2] = jnp.dot(
                cotf[...], wcols[t % 2], preferred_element_type=f32
            ).astype(jnp.bfloat16)
            store_hgrad(t).start()

        @pl.when(s < n)
        def _():
            send_y(s).start()

        @pl.when(jnp.logical_and(s >= Y_LAG, s < n + Y_LAG))
        def _():
            k = s - Y_LAG
            send_y(k).wait_recv()

            @pl.when(k >= SLOTS)
            def _():
                send_mirror(k - SLOTS).wait_send()

            total = jnp.dot(cot_own[1], tok[k], preferred_element_type=f32)
            total = total + decode(yrecv[k, 1], scales[0, 0:1, 0:1])
            msend[k % SLOTS] = encode(total, scales[1, 0:1, 0:1])

        @pl.when(s >= Z_LAG)
        def _():
            k = s - Z_LAG

            @pl.when(k >= 2)
            def _():
                store_wgrad(k - 2).wait()

            total = jnp.dot(cot_own[0], tok[k], preferred_element_type=f32)
            wstage[k % 2] = total + decode(yrecv[k, 0], scales[0, 0:1, 0:1])

        @pl.when(jnp.logical_and(s >= Y_LAG, s < n + Y_LAG))
        def _():
            send_mirror(s - Y_LAG).start()

        @pl.when(s >= Z_LAG)
        def _():
            k = s - Z_LAG
            send_mirror(k).wait_recv()
            both = wstage[k % 2] + decode(mrecv[k], scales[0, 0:1, 0:1])
            wstage[k % 2] = both * grad_scale
            store_wgrad(k).start()

    core_part[1].wait_recv()
    x_part.wait_recv()

    @pl.loop(0, per_block)
    def _(k):
        at = pl.ds(pl.multiple_of(k * CHUNK, CHUNK), CHUNK)
        ostage[:, at] = (part[3, :, at] + crecv[1, :, at] + xrecv[:, at]).astype(jnp.bfloat16)

    store_out = pltpu.make_async_copy(ostage, out, load_sem.at[2])
    store_out.start()

    for i in range(2):
        store_wgrad(n - 2 + i).wait()
        store_hgrad(n - 2 + i).wait()
    for k in range(SLOTS):
        send_y(n - SLOTS + k).wait_send()
        send_mirror(n - SLOTS + k).wait_send()

    @pl.loop(0, n)
    def _(s):
        send_tokens(s).wait_send()

    for i in range(5):
        exchange(i).wait_send()
    core_own.wait_send()
    x_own.wait_send()
    core_relay.wait_send()
    core_peer.wait_send()
    core_part[0].wait_send()
    core_part[1].wait_send()
    x_part.wait_send()

    @pl.when(chosen)
    def _():
        x_peer.wait_send()

    @pl.when(jnp.logical_not(chosen))
    def _():
        z_cot.wait_send()

    store_out.wait()


def shards_mirror(hidden, weight, cotangent):
    rows, width = hidden.shape
    block = cotangent.shape[1]
    features = weight.shape[0]
    n = width // CHUNK
    f32, bf16 = jnp.float32, jnp.bfloat16
    grad_scale = float(rows * lax.axis_size("gx")) ** (-0.5)
    dma = pltpu.SemaphoreType.DMA
    return pl.pallas_call(
        functools.partial(mirror_kernel, grad_scale),
        out_shape=(
            jax.ShapeDtypeStruct((rows, block), bf16),
            jax.ShapeDtypeStruct((rows, width), bf16),
            jax.ShapeDtypeStruct((block // 2, width), f32),
        ),
        in_specs=[pl.BlockSpec(memory_space=pl.ANY)] * 3,
        out_specs=[pl.BlockSpec(memory_space=pl.ANY)] * 3,
        scratch_shapes=[
            pltpu.VMEM((rows, width), bf16),
            pltpu.VMEM((n, 2 * rows, CHUNK), bf16),
            pltpu.VMEM((rows, features), bf16),
            pltpu.VMEM((2, rows, block), bf16),
            pltpu.VMEM((2, block // 2, 2 * rows), bf16),
            pltpu.VMEM((2, block // 2, 2 * rows), bf16),
            pltpu.VMEM((2, CHUNK, width), bf16),
            pltpu.VMEM((2, features, CHUNK), bf16),
            pltpu.VMEM((4, rows, block), f32),
            pltpu.VMEM((2, rows, block), f32),
            pltpu.VMEM((rows, block), f32),
            pltpu.VMEM((SLOTS, 2, block // 2, CHUNK), bf16),
            pltpu.VMEM((n, 2, block // 2, CHUNK), bf16),
            pltpu.VMEM((SLOTS, block // 2, CHUNK), bf16),
            pltpu.VMEM((n, block // 2, CHUNK), bf16),
            pltpu.VMEM((2, block // 2, CHUNK), f32),
            pltpu.VMEM((2, rows, CHUNK), bf16),
            pltpu.VMEM((rows, block), bf16),
            pltpu.VMEM((6, 16, LANES), f32),
            pltpu.VMEM((5, 16, LANES), f32),
            pltpu.VMEM((2, 8, LANES), f32),
            dma((3,)), dma((n,)), dma((2,)), dma((2,)), dma((5,)), dma((5,)), dma((4,)), dma((4,)),
            dma((n,)), dma((n,)), dma((n,)), dma((n,)), dma((n,)), dma((n,)), dma((5,)), dma((5,)),
            dma((2,)), dma((2,)),
        ],
        compiler_params=pltpu.CompilerParams(
            collective_id=0, has_side_effects=True, vmem_limit_bytes=67_000_000
        ),
        name="mirror",
    )(hidden, weight, cotangent)


def solution(mesh):
    shape = dict(mesh.shape)
    mirror = shape["gx"] == 8 and shape["gy"] == 4
    return jax.shard_map(
        shards_mirror if mirror else shards_ring,
        mesh=mesh,
        in_specs=(P("gx", "gy"), P(None, "gy"), P("gx", "gy")),
        out_specs=(P("gx", "gy"), P("gx", "gy"), P("gx", "gy")),
        check_vma=False,
    )
```

```python
import functools

import jax
import jax.numpy as jnp
from jax import lax
from jax.experimental import pallas as pl
from jax.experimental.pallas import tpu as pltpu
from jax.sharding import PartitionSpec as P


PAIR = 2
STREAMS = 4
LANES = 128


def cuts(width, pieces):
    units = width // LANES if width % LANES == 0 else width
    step = width // units
    pieces = min(pieces, units)
    edges = [units * i // pieces * step for i in range(pieces + 1)]
    return list(zip(edges[:-1], edges[1:]))


def dot_t(a, b):
    return lax.dot_general(a, b, (((0,), (0,)), ((), ())), preferred_element_type=jnp.float32)


def shards_ring(hidden, weight, cotangent):
    gx, gy = lax.axis_size("gx"), lax.axis_size("gy")
    nz, nx = gx // PAIR, gy // PAIR
    ix, iy = lax.axis_index("gx"), lax.axis_index("gy")
    z, y = ix // PAIR, ix % PAIR
    x, core = iy // PAIR, iy % PAIR
    rows, width = hidden.shape
    block = cotangent.shape[1]
    features = weight.shape[0]
    grad_scale = float(rows * gx) ** (-0.5)
    f32 = jnp.float32

    def z_shift(v, d):
        return lax.ppermute(v, "gx", [(g, (g + PAIR * d) % gx) for g in range(gx)])

    def y_swap(v):
        return lax.ppermute(v, "gx", [(g, g ^ 1) for g in range(gx)])

    def x_shift(v, d):
        return lax.ppermute(v, "gy", [(j, (j + PAIR * d) % gy) for j in range(gy)])

    def core_swap(v):
        return lax.ppermute(v, "gy", [(j, j ^ 1) for j in range(gy)])

    mine = jnp.stack([cotangent] + [x_shift(cotangent, d) for d in range(1, nx)])
    theirs = core_swap(mine)
    full = jnp.zeros((rows, features), cotangent.dtype)
    for d in range(nx):
        source = (x - d) % nx * PAIR
        full = lax.dynamic_update_slice(full, mine[d], (0, (source + core) * block))
        full = lax.dynamic_update_slice(full, theirs[d], (0, (source + 1 - core) * block))

    span = features // nz
    half = rows // PAIR
    fetched = jnp.stack(
        [
            z_shift(
                lax.dynamic_slice(full, (core * half, (z + t) % nz * span), (half, span)), t
            )
            for t in range(1, nz)
        ]
    )
    other = core_swap(fetched)
    low = jnp.where(core == 0, fetched, other)
    high = jnp.where(core == 0, other, fetched)
    by_shift = [lax.dynamic_slice(full, (0, z * span), (rows, span))]
    by_shift += [jnp.concatenate([low[t], high[t]]) for t in range(nz - 1)]
    rows_out = span // PAIR

    def of_feature_block(stack, which):
        return lax.dynamic_slice(stack, (0, which * rows_out), (rows * nz, rows_out))

    stacks = (
        jnp.concatenate(by_shift),
        jnp.concatenate([by_shift[-t % nz] for t in range(nz)]),
    )
    own = [of_feature_block(s, y) for s in stacks]
    peer = [of_feature_block(s, 1 - y) for s in stacks]

    partial = lax.dot_general(
        hidden, weight, (((1,), (1,)), ((), ())), preferred_element_type=f32
    )

    def columns(which_core):
        return jnp.stack(
            [
                lax.dynamic_slice(
                    partial, (0, ((x + d) % nx * PAIR + which_core) * block), (rows, block)
                )
                for d in range(nx)
            ]
        )

    chip_sum = columns(core) + core_swap(columns(1 - core))
    total = chip_sum[0]
    for d in range(1, nx):
        total = total + x_shift(chip_sum[d], d)
    output = total.astype(jnp.bfloat16)

    hidden_grad = jnp.dot(full, weight, preferred_element_type=f32).astype(jnp.bfloat16)

    weight_grad = jnp.zeros((rows_out, width), f32)
    for s, (start, stop) in enumerate(cuts(width, STREAMS)):
        way = 1 if s % 2 == 0 else -1
        held = [hidden[:, start:stop]]
        for _ in range(nz - 1):
            held.append(z_shift(held[-1], way))
        tokens = jnp.concatenate(held)
        arrived = y_swap(dot_t(peer[s % 2], tokens))
        summed = dot_t(own[s % 2], tokens) + arrived
        weight_grad = lax.dynamic_update_slice(weight_grad, summed * grad_scale, (0, start))
    return (output, hidden_grad, weight_grad)


MESH = pl.DeviceIdType.MESH
CHUNK = 2 * LANES
AHEAD = 1
Z_LAG = 3
HG_LAG = 3
OUT_LAG = 4
OUT_END = 9
T_AT = 5
SLOTS = 4
TOP = 2.0 ** 25


def encode(value, inverse_step):
    u = value * inverse_step
    square = u * u
    return (square * square * u).astype(jnp.bfloat16)


def decode(code, step):
    code = code.astype(jnp.float32)
    root = jnp.exp2(jnp.log2(jnp.maximum(jnp.abs(code), 1e-37)) * 0.2) * step
    return jnp.where(code > 0, root, jnp.where(code < 0, -root, 0.0))


def mirror_kernel(
    grad_scale, hidden, weight, cot, out, hgrad, wgrad,
    hid, tok, cotf, cotp, cot_peer, cot_own, wtile, wcols, part, crecv, xrecv,
    ysend, yrecv, msend, mrecv, maxima, arrived, scales,
    load_sem, wt_sem, wc_sem, c_send, c_recv, x_send, x_recv,
    t_send, t_recv, y_send, y_recv, m_send, m_recv, b_send, b_recv,
):
    f32 = jnp.float32
    ix, iy = lax.axis_index("gx"), lax.axis_index("gy")
    z, y = ix // 2, ix % 2
    x, core = iy // 2, iy % 2
    rows, width = hid.shape
    block = cotf.shape[1] // 4
    half = block // 2
    n = width // CHUNK
    per_block = block // CHUNK
    n_early = 2 * per_block

    to_core = (ix, x * 2 + 1 - core)
    to_x = (ix, (1 - x) * 2 + core)
    to_y = (z * 2 + 1 - y, iy)
    pair = z + 1 - 2 * (z % 2)
    mirror = 3 - z
    to_pair = (pair * 2 + y, iy)
    to_mirror = (mirror * 2 + y, iy)
    chosen = jnp.logical_or(iy == z, iy == 3 - z)
    other = jnp.logical_not(chosen)
    x_block = (1 - x) * 2 + core

    def remote(src, dst, send, recv, device):
        return pltpu.make_async_remote_copy(
            src_ref=src, dst_ref=dst, send_sem=send, recv_sem=recv,
            device_id=device, device_id_type=MESH,
        )

    def lanes(start, size):
        return pl.ds(pl.multiple_of(start, size), size)

    def cols(ref, s):
        return ref.at[:, lanes(s * CHUNK, CHUNK)]

    def piece(p):
        return (1 - y if p == 0 else y) * half

    def of_block(j, p):
        return cotf.at[:, lanes(j * block + piece(p), half)]

    def of_peer(slot, p):
        return cotp.at[slot, :, lanes(piece(p), half)]

    def of_cot(p):
        return cot.at[:, lanes(piece(p), half)]

    first = jnp.where(jnp.where(chosen, iy, x_block) == z, 0, 1)
    peer_slot = jnp.where(iy == z, 0, 1)
    relay_slot = jnp.where(iy == pair, 0, 1)
    own_block = cotf.at[:, lanes(iy * block, block)]
    core_own = remote(cot, own_block, c_send.at[0], c_recv.at[0], to_core)
    x_own, z_cot, x_peer, core_relay, core_peer = [], [], [], [], []
    for p in range(2):
        x_own.append(remote(of_cot(p), of_block(iy, p), x_send.at[p], x_recv.at[p], to_x))
        z_cot.append(
            remote(of_cot(p), of_peer(relay_slot, p), x_send.at[2 + p], x_recv.at[2 + p], to_pair)
        )
        mine = of_peer(peer_slot, p)
        x_peer.append(remote(mine, mine, x_send.at[4 + p], x_recv.at[4 + p], to_x))
        mine = of_block(x_block, p)
        core_relay.append(remote(mine, mine, c_send.at[3 + p], c_recv.at[3 + p], to_core))
        mine = of_peer(first, p)
        core_peer.append(remote(mine, mine, c_send.at[5 + p], c_recv.at[5 + p], to_core))
    core_part = [
        remote(part.at[2 * i], crecv.at[i], c_send.at[1 + i], c_recv.at[1 + i], to_core)
        for i in range(2)
    ]
    x_part = remote(part.at[1], xrecv, x_send.at[6], x_recv.at[6], to_x)

    def send_tokens(s):
        return remote(cols(hidden, s), tok.at[s], t_send.at[s], t_recv.at[s], to_pair)

    def send_y(s, r):
        return remote(
            ysend.at[s % SLOTS, r], yrecv.at[s, r], y_send.at[s, r], y_recv.at[s, r], to_y
        )

    def send_mirror(s):
        return remote(msend.at[s % SLOTS], mrecv.at[s], m_send.at[s], m_recv.at[s], to_mirror)

    def load_rows(t):
        q, sub = t // per_block, t % per_block
        b = jnp.where(
            q == 0, 3 - iy, jnp.where(q == 1, x_block, jnp.where(q == 2, x * 2 + 1 - core, iy))
        )
        at = pl.multiple_of(b * block + sub * CHUNK, CHUNK)
        return pltpu.make_async_copy(
            weight.at[pl.ds(at, CHUNK)], wtile.at[t % 2], wt_sem.at[t % 2]
        )

    def rows_product(t):
        return lax.dot_general(
            hid[...], wtile[t % 2], (((1,), (1,)), ((), ())), preferred_element_type=f32
        )

    def load_cols(t):
        return pltpu.make_async_copy(cols(weight, t), wcols.at[t % 2], wc_sem.at[t % 2])

    def product(lhs, s):
        mine = jnp.dot(lhs[:, :rows], hid[:, lanes(s * CHUNK, CHUNK)], preferred_element_type=f32)
        return mine + jnp.dot(lhs[:, rows:], tok[s], preferred_element_type=f32)

    load_hidden = pltpu.make_async_copy(hidden, hid, load_sem.at[0])
    load_cot = pltpu.make_async_copy(cot, own_block, load_sem.at[1])
    load_hidden.start()
    load_cot.start()
    load_rows(0).start()

    barrier = pltpu.get_barrier_semaphore()
    for device in (to_core, to_x, to_y, to_pair, to_mirror):
        pl.semaphore_signal(barrier, inc=1, device_id=device, device_id_type=MESH)
    pl.semaphore_wait(barrier, 5)

    @pl.when(chosen)
    def _():
        x_own[0].start()
        x_own[1].start()

    @pl.when(other)
    def _():
        z_cot[0].start()
        z_cot[1].start()

    core_own.start()
    load_hidden.wait()
    load_cot.wait()

    stages = (to_core, to_x, to_pair, to_mirror, to_y)

    def exchange(i):
        return remote(maxima.at[i], arrived.at[i], b_send.at[i], b_recv.at[i], stages[i])

    def settle(i):
        exchange(i).wait_recv()
        maxima[i + 1] = jnp.maximum(maxima[i], arrived[i])

    def highest(ref, start, count):
        def body(i, best):
            v = jnp.abs(ref[:, lanes(start + i * CHUNK, CHUNK)].astype(f32))
            return jnp.maximum(best, jnp.max(v.reshape(rows // 8, 8, CHUNK), axis=0))

        best = lax.fori_loop(0, count, body, jnp.zeros((8, CHUNK), f32))
        return jnp.full((8, LANES), jnp.max(best), f32)

    @pl.loop(0, n_early)
    def _(t):
        q, sub = t // per_block, t % per_block

        @pl.when(t + 1 < n_early)
        def _():
            load_rows(t + 1).start()

        @pl.when(t == 1)
        def _():
            maxima[0, 0:8] = highest(hid, 0, n)
            maxima[0, 8:16] = highest(cotf, iy * block, per_block)

        for i in range(5):
            @pl.when(t == 3 + i)
            def _():
                settle(i)

        @pl.when(t == per_block)
        def _():
            @pl.when(chosen)
            def _():
                z_cot[0].wait_recv()
                x_peer[0].start()
                core_peer[0].start()

            @pl.when(other)
            def _():
                x_own[0].wait_recv()
                core_relay[0].start()

        load_rows(t).wait()
        part[q, :, lanes(sub * CHUNK, CHUNK)] = rows_product(t)

        for i in range(5):
            @pl.when(t == 2 + i)
            def _():
                exchange(i).start()

        @pl.when(t == per_block)
        def _():
            core_part[0].start()

        @pl.when(t == T_AT)
        def _():
            send_tokens(0).start()

    load_rows(n_early).start()
    load_cols(0).start()
    core_part[0].wait_recv()

    @pl.loop(0, per_block)
    def _(k):
        at = lanes(k * CHUNK, CHUNK)
        part[1, :, at] = part[1, :, at] + crecv[0, :, at]

    best = maxima[5]
    step = jnp.maximum(best[0:8] * best[8:16] * (4.0 * rows / TOP), 1e-36)
    scales[0] = step
    scales[1] = 1.0 / step

    @pl.when(chosen)
    def _():
        z_cot[1].wait_recv()
        x_peer[1].start()
        core_peer[1].start()

    @pl.when(other)
    def _():
        x_own[1].wait_recv()
        core_relay[1].start()

    for s in range(1, AHEAD):
        send_tokens(s).start()

    def turn(dst, p):
        for r in range(2):
            j = z if r == 0 else 3 - z
            dst[r, :, :rows] = cotf[:, lanes(j * block + piece(p), half)].T
            dst[r, :, rows:] = cotp[r, :, lanes(piece(p), half)].T

    core_own.wait_recv()

    @pl.when(chosen)
    def _():
        core_relay[0].wait_recv()

    @pl.when(other)
    def _():
        x_peer[0].wait_recv()
        core_peer[0].start()

    core_peer[0].wait_recv()
    turn(cot_peer, 0)


    @pl.loop(0, n + Z_LAG)
    def _(s):
        @pl.when(s + AHEAD < n)
        def _():
            send_tokens(s + AHEAD).start()

        @pl.when(s == 1)
        def _():
            @pl.when(chosen)
            def _():
                core_relay[1].wait_recv()

            @pl.when(other)
            def _():
                x_peer[1].wait_recv()
                core_peer[1].start()

            core_peer[1].wait_recv()
            turn(cot_own, 1)

            @pl.when(other)
            def _():
                x_own[0].start()
                x_own[1].start()

        @pl.when(jnp.logical_and(s >= 1, s <= n))
        def _():
            k = s - 1
            send_y(k, 1).wait_recv()

            @pl.when(k >= SLOTS)
            def _():
                send_mirror(k - SLOTS).wait_send()

            total = product(cot_own.at[1], k) + decode(yrecv[k, 1], scales[0, 0:1, 0:1])
            msend[k % SLOTS] = encode(total, scales[1, 0:1, 0:1])

        @pl.when(s < n)
        def _():
            send_tokens(s).wait_recv()

            @pl.when(s >= SLOTS)
            def _():
                send_y(s - SLOTS, 0).wait_send()
                send_y(s - SLOTS, 1).wait_send()

            ysend[s % SLOTS, 1] = encode(product(cot_peer.at[1], s), scales[1, 0:1, 0:1])

            @pl.when(s >= 1)
            def _():
                send_mirror(s - 1).start()

            ysend[s % SLOTS, 0] = encode(product(cot_peer.at[0], s), scales[1, 0:1, 0:1])
            send_y(s, 1).start()

        @pl.when(s >= Z_LAG)
        def _():
            k = s - Z_LAG

            send_y(k, 0).wait_recv()
            total = product(cot_own.at[0], k)
            total = total + decode(yrecv[k, 0], scales[0, 0:1, 0:1])
            wgrad[:, lanes(k * CHUNK, CHUNK)] = total

        @pl.when(s == n)
        def _():
            send_mirror(s - 1).start()

        @pl.when(s == 2)
        def _():
            x_part.start()

        @pl.when(s == HG_LAG)
        def _():
            for p in range(2):
                @pl.when(chosen)
                def _():
                    x_own[p].wait_recv()
                    core_relay[p].start()

            for p in range(2):
                @pl.when(other)
                def _():
                    core_relay[p].wait_recv()

        @pl.when(jnp.logical_and(s >= HG_LAG, s < n + HG_LAG))
        def _():
            t = s - HG_LAG

            @pl.when(t + 1 < n)
            def _():
                load_cols(t + 1).start()

            load_cols(t).wait()

            hgrad[:, lanes(t * CHUNK, CHUNK)] = jnp.dot(
                cotf[...], wcols[t % 2], preferred_element_type=f32
            ).astype(jnp.bfloat16)

        @pl.when(s < n)
        def _():
            send_y(s, 0).start()

        @pl.when(jnp.logical_and(s >= OUT_LAG, s < OUT_LAG + per_block))
        def _():
            t = n_early + s - OUT_LAG
            load_rows(t + 1).start()
            load_rows(t).wait()
            part[2, :, lanes((s - OUT_LAG) * CHUNK, CHUNK)] = rows_product(t)

        @pl.when(s == OUT_LAG + per_block)
        def _():
            core_part[1].start()

        @pl.when(s == OUT_END)
        def _():
            core_part[1].wait_recv()
            x_part.wait_recv()

        @pl.when(jnp.logical_and(s >= OUT_END, s < OUT_END + per_block))
        def _():
            k = s - OUT_END
            t = n_early + per_block + k

            @pl.when(k + 1 < per_block)
            def _():
                load_rows(t + 1).start()

            load_rows(t).wait()
            at = lanes(k * CHUNK, CHUNK)
            total = rows_product(t) + crecv[1, :, at] + xrecv[:, at]
            out[:, at] = total.astype(jnp.bfloat16)

        @pl.when(s >= Z_LAG)
        def _():
            k = s - Z_LAG
            send_mirror(k).wait_recv()
            at = lanes(k * CHUNK, CHUNK)
            wgrad[:, at] = (wgrad[:, at] + decode(mrecv[k], scales[0, 0:1, 0:1])) * grad_scale

    for k in range(SLOTS):
        send_y(n - SLOTS + k, 0).wait_send()
        send_y(n - SLOTS + k, 1).wait_send()
        send_mirror(n - SLOTS + k).wait_send()

    @pl.loop(0, n)
    def _(s):
        send_tokens(s).wait_send()

    for i in range(5):
        exchange(i).wait_send()
    core_own.wait_send()
    core_part[0].wait_send()
    core_part[1].wait_send()
    x_part.wait_send()
    for p in range(2):
        x_own[p].wait_send()
        core_relay[p].wait_send()
        core_peer[p].wait_send()

        @pl.when(chosen)
        def _():
            x_peer[p].wait_send()

        @pl.when(other)
        def _():
            z_cot[p].wait_send()


def shards_mirror(hidden, weight, cotangent):
    rows, width = hidden.shape
    block = cotangent.shape[1]
    features = weight.shape[0]
    n = width // CHUNK
    f32, bf16 = jnp.float32, jnp.bfloat16
    grad_scale = float(rows * lax.axis_size("gx")) ** (-0.5)
    dma = pltpu.SemaphoreType.DMA
    return pl.pallas_call(
        functools.partial(mirror_kernel, grad_scale),
        out_shape=(
            pltpu.VMEM((rows, block), bf16),
            pltpu.VMEM((rows, width), bf16),
            pltpu.VMEM((block // 2, width), f32),
        ),
        in_specs=[pl.BlockSpec(memory_space=pl.ANY)] * 3,
        out_specs=[pl.BlockSpec(memory_space=pltpu.VMEM)] * 3,
        scratch_shapes=[
            pltpu.VMEM((rows, width), bf16),
            pltpu.VMEM((n, rows, CHUNK), bf16),
            pltpu.VMEM((rows, features), bf16),
            pltpu.VMEM((2, rows, block), bf16),
            pltpu.VMEM((2, block // 2, 2 * rows), bf16),
            pltpu.VMEM((2, block // 2, 2 * rows), bf16),
            pltpu.VMEM((2, CHUNK, width), bf16),
            pltpu.VMEM((2, features, CHUNK), bf16),
            pltpu.VMEM((3, rows, block), f32),
            pltpu.VMEM((2, rows, block), f32),
            pltpu.VMEM((rows, block), f32),
            pltpu.VMEM((SLOTS, 2, block // 2, CHUNK), bf16),
            pltpu.VMEM((n, 2, block // 2, CHUNK), bf16),
            pltpu.VMEM((SLOTS, block // 2, CHUNK), bf16),
            pltpu.VMEM((n, block // 2, CHUNK), bf16),
            pltpu.VMEM((6, 16, LANES), f32),
            pltpu.VMEM((5, 16, LANES), f32),
            pltpu.VMEM((2, 8, LANES), f32),
            dma((2,)), dma((2,)), dma((2,)), dma((7,)), dma((7,)), dma((7,)), dma((7,)),
            dma((n,)), dma((n,)), dma((n, 2)), dma((n, 2)), dma((n,)), dma((n,)), dma((5,)),
            dma((5,)),
        ],
        compiler_params=pltpu.CompilerParams(
            collective_id=0, has_side_effects=True, vmem_limit_bytes=54_900_000
        ),
        name="mirror",
    )(hidden, weight, cotangent)


def solution(mesh):
    shape = dict(mesh.shape)
    mirror = shape["gx"] == 8 and shape["gy"] == 4
    return jax.shard_map(
        shards_mirror if mirror else shards_ring,
        mesh=mesh,
        in_specs=(P("gx", "gy"), P(None, "gy"), P("gx", "gy")),
        out_specs=(P("gx", "gy"), P("gx", "gy"), P("gx", "gy")),
        check_vma=False,
    )
```

```python
import functools

import jax
import jax.numpy as jnp
from jax import lax
from jax.experimental import pallas as pl
from jax.experimental.pallas import tpu as pltpu
from jax.sharding import PartitionSpec as P


PAIR = 2
STREAMS = 4
LANES = 128


def cuts(width, pieces):
    units = width // LANES if width % LANES == 0 else width
    step = width // units
    pieces = min(pieces, units)
    edges = [units * i // pieces * step for i in range(pieces + 1)]
    return list(zip(edges[:-1], edges[1:]))


def dot_t(a, b):
    return lax.dot_general(a, b, (((0,), (0,)), ((), ())), preferred_element_type=jnp.float32)


def shards_ring(hidden, weight, cotangent):
    gx, gy = lax.axis_size("gx"), lax.axis_size("gy")
    nz, nx = gx // PAIR, gy // PAIR
    ix, iy = lax.axis_index("gx"), lax.axis_index("gy")
    z, y = ix // PAIR, ix % PAIR
    x, core = iy // PAIR, iy % PAIR
    rows, width = hidden.shape
    block = cotangent.shape[1]
    features = weight.shape[0]
    grad_scale = float(rows * gx) ** (-0.5)
    f32 = jnp.float32

    def z_shift(v, d):
        return lax.ppermute(v, "gx", [(g, (g + PAIR * d) % gx) for g in range(gx)])

    def y_swap(v):
        return lax.ppermute(v, "gx", [(g, g ^ 1) for g in range(gx)])

    def x_shift(v, d):
        return lax.ppermute(v, "gy", [(j, (j + PAIR * d) % gy) for j in range(gy)])

    def core_swap(v):
        return lax.ppermute(v, "gy", [(j, j ^ 1) for j in range(gy)])

    mine = jnp.stack([cotangent] + [x_shift(cotangent, d) for d in range(1, nx)])
    theirs = core_swap(mine)
    full = jnp.zeros((rows, features), cotangent.dtype)
    for d in range(nx):
        source = (x - d) % nx * PAIR
        full = lax.dynamic_update_slice(full, mine[d], (0, (source + core) * block))
        full = lax.dynamic_update_slice(full, theirs[d], (0, (source + 1 - core) * block))

    span = features // nz
    half = rows // PAIR
    fetched = jnp.stack(
        [
            z_shift(
                lax.dynamic_slice(full, (core * half, (z + t) % nz * span), (half, span)), t
            )
            for t in range(1, nz)
        ]
    )
    other = core_swap(fetched)
    low = jnp.where(core == 0, fetched, other)
    high = jnp.where(core == 0, other, fetched)
    by_shift = [lax.dynamic_slice(full, (0, z * span), (rows, span))]
    by_shift += [jnp.concatenate([low[t], high[t]]) for t in range(nz - 1)]
    rows_out = span // PAIR

    def of_feature_block(stack, which):
        return lax.dynamic_slice(stack, (0, which * rows_out), (rows * nz, rows_out))

    stacks = (
        jnp.concatenate(by_shift),
        jnp.concatenate([by_shift[-t % nz] for t in range(nz)]),
    )
    own = [of_feature_block(s, y) for s in stacks]
    peer = [of_feature_block(s, 1 - y) for s in stacks]

    partial = lax.dot_general(
        hidden, weight, (((1,), (1,)), ((), ())), preferred_element_type=f32
    )

    def columns(which_core):
        return jnp.stack(
            [
                lax.dynamic_slice(
                    partial, (0, ((x + d) % nx * PAIR + which_core) * block), (rows, block)
                )
                for d in range(nx)
            ]
        )

    chip_sum = columns(core) + core_swap(columns(1 - core))
    total = chip_sum[0]
    for d in range(1, nx):
        total = total + x_shift(chip_sum[d], d)
    output = total.astype(jnp.bfloat16)

    hidden_grad = jnp.dot(full, weight, preferred_element_type=f32).astype(jnp.bfloat16)

    weight_grad = jnp.zeros((rows_out, width), f32)
    for s, (start, stop) in enumerate(cuts(width, STREAMS)):
        way = 1 if s % 2 == 0 else -1
        held = [hidden[:, start:stop]]
        for _ in range(nz - 1):
            held.append(z_shift(held[-1], way))
        tokens = jnp.concatenate(held)
        arrived = y_swap(dot_t(peer[s % 2], tokens))
        summed = dot_t(own[s % 2], tokens) + arrived
        weight_grad = lax.dynamic_update_slice(weight_grad, summed * grad_scale, (0, start))
    return (output, hidden_grad, weight_grad)


MESH = pl.DeviceIdType.MESH
CHUNK = 2 * LANES
AHEAD = 1
Z_LAG = 3
HG_LAG = 3
OUT_LAG = 4
OUT_END = 9
T_AT = 5
SLOTS = 4
TOP = 2.0 ** 25


def encode(value, inverse_step):
    u = value * inverse_step
    square = u * u
    return (square * square * u).astype(jnp.bfloat16)


def decode(code, step):
    code = code.astype(jnp.float32)
    root = jnp.exp2(jnp.log2(jnp.maximum(jnp.abs(code), 1e-37)) * 0.2) * step
    return jnp.where(code > 0, root, jnp.where(code < 0, -root, 0.0))


def mirror_kernel(
    grad_scale, hidden, weight, cot, out, hgrad, wgrad,
    hid, tok, cotf, cotp, cot_peer, cot_own, wtile, wcols, part, crecv, xrecv,
    ysend, yrecv, msend, mrecv, maxima, arrived, scales,
    load_sem, wt_sem, wc_sem, c_send, c_recv, x_send, x_recv,
    t_send, t_recv, y_send, y_recv, m_send, m_recv, b_send, b_recv,
):
    f32 = jnp.float32
    ix, iy = lax.axis_index("gx"), lax.axis_index("gy")
    z, y = ix // 2, ix % 2
    x, core = iy // 2, iy % 2
    rows, width = hid.shape
    block = cotf.shape[1] // 4
    half = block // 2
    n = width // CHUNK
    per_block = block // CHUNK
    n_early = 2 * per_block

    to_core = (ix, x * 2 + 1 - core)
    to_x = (ix, (1 - x) * 2 + core)
    to_y = (z * 2 + 1 - y, iy)
    pair = z + 1 - 2 * (z % 2)
    mirror = 3 - z
    to_pair = (pair * 2 + y, iy)
    to_mirror = (mirror * 2 + y, iy)
    chosen = jnp.logical_or(iy == z, iy == 3 - z)
    other = jnp.logical_not(chosen)
    x_block = (1 - x) * 2 + core

    def remote(src, dst, send, recv, device):
        return pltpu.make_async_remote_copy(
            src_ref=src, dst_ref=dst, send_sem=send, recv_sem=recv,
            device_id=device, device_id_type=MESH,
        )

    def lanes(start, size):
        return pl.ds(pl.multiple_of(start, size), size)

    def cols(ref, s):
        return ref.at[:, lanes(s * CHUNK, CHUNK)]

    def piece(p):
        return (1 - y if p == 0 else y) * half

    def of_block(j, p):
        return cotf.at[:, lanes(j * block + piece(p), half)]

    def of_peer(slot, p):
        return cotp.at[slot, :, lanes(piece(p), half)]

    def of_cot(p):
        return cot.at[:, lanes(piece(p), half)]

    first = jnp.where(jnp.where(chosen, iy, x_block) == z, 0, 1)
    peer_slot = jnp.where(iy == z, 0, 1)
    relay_slot = jnp.where(iy == pair, 0, 1)
    own_block = cotf.at[:, lanes(iy * block, block)]
    core_own = remote(cot, own_block, c_send.at[0], c_recv.at[0], to_core)
    x_own, z_cot, x_peer, core_relay, core_peer = [], [], [], [], []
    for p in range(2):
        x_own.append(remote(of_cot(p), of_block(iy, p), x_send.at[p], x_recv.at[p], to_x))
        z_cot.append(
            remote(of_cot(p), of_peer(relay_slot, p), x_send.at[2 + p], x_recv.at[2 + p], to_pair)
        )
        mine = of_peer(peer_slot, p)
        x_peer.append(remote(mine, mine, x_send.at[4 + p], x_recv.at[4 + p], to_x))
        mine = of_block(x_block, p)
        core_relay.append(remote(mine, mine, c_send.at[3 + p], c_recv.at[3 + p], to_core))
        mine = of_peer(first, p)
        core_peer.append(remote(mine, mine, c_send.at[5 + p], c_recv.at[5 + p], to_core))
    core_part = [
        remote(part.at[2 * i], crecv.at[i], c_send.at[1 + i], c_recv.at[1 + i], to_core)
        for i in range(2)
    ]
    x_part = remote(part.at[1], xrecv, x_send.at[6], x_recv.at[6], to_x)

    def send_tokens(s):
        return remote(cols(hidden, s), tok.at[s], t_send.at[s], t_recv.at[s], to_pair)

    def send_y(s, r):
        return remote(
            ysend.at[s % SLOTS, r], yrecv.at[s, r], y_send.at[s, r], y_recv.at[s, r], to_y
        )

    def send_mirror(s):
        return remote(msend.at[s % SLOTS], mrecv.at[s], m_send.at[s], m_recv.at[s], to_mirror)

    def load_rows(t):
        q, sub = t // per_block, t % per_block
        b = jnp.where(
            q == 0, 3 - iy, jnp.where(q == 1, x_block, jnp.where(q == 2, x * 2 + 1 - core, iy))
        )
        at = pl.multiple_of(b * block + sub * CHUNK, CHUNK)
        return pltpu.make_async_copy(
            weight.at[pl.ds(at, CHUNK)], wtile.at[t % 2], wt_sem.at[t % 2]
        )

    def rows_product(t):
        return lax.dot_general(
            hid[...], wtile[t % 2], (((1,), (1,)), ((), ())), preferred_element_type=f32
        )

    def load_cols(t):
        return pltpu.make_async_copy(cols(weight, t), wcols.at[t % 2], wc_sem.at[t % 2])

    def product(lhs, s):
        mine = jnp.dot(lhs[:, :rows], hid[:, lanes(s * CHUNK, CHUNK)], preferred_element_type=f32)
        return mine + jnp.dot(lhs[:, rows:], tok[s], preferred_element_type=f32)

    load_hidden = pltpu.make_async_copy(hidden, hid, load_sem.at[0])
    load_cot = pltpu.make_async_copy(cot, own_block, load_sem.at[1])
    load_hidden.start()
    load_cot.start()
    load_rows(0).start()

    barrier = pltpu.get_barrier_semaphore()
    for device in (to_core, to_x, to_y, to_pair, to_mirror):
        pl.semaphore_signal(barrier, inc=1, device_id=device, device_id_type=MESH)
    pl.semaphore_wait(barrier, 5)

    @pl.when(chosen)
    def _():
        x_own[0].start()
        x_own[1].start()

    @pl.when(other)
    def _():
        z_cot[0].start()
        z_cot[1].start()

    core_own.start()
    load_hidden.wait()
    load_cot.wait()

    stages = (to_core, to_x, to_pair, to_mirror, to_y)

    def exchange(i):
        return remote(maxima.at[i], arrived.at[i], b_send.at[i], b_recv.at[i], stages[i])

    def settle(i):
        exchange(i).wait_recv()
        maxima[i + 1] = jnp.maximum(maxima[i], arrived[i])

    def highest(ref, start, count):
        def body(i, best):
            v = jnp.abs(ref[:, lanes(start + i * CHUNK, CHUNK)].astype(f32))
            return jnp.maximum(best, jnp.max(v.reshape(rows // 8, 8, CHUNK), axis=0))

        best = lax.fori_loop(0, count, body, jnp.zeros((8, CHUNK), f32))
        return jnp.full((8, LANES), jnp.max(best), f32)

    @pl.loop(0, n_early)
    def _(t):
        q, sub = t // per_block, t % per_block

        @pl.when(t + 1 < n_early)
        def _():
            load_rows(t + 1).start()

        @pl.when(t == 1)
        def _():
            maxima[0, 0:8] = highest(hid, 0, n)
            maxima[0, 8:16] = highest(cotf, iy * block, per_block)

        for i in range(5):
            @pl.when(t == 3 + i)
            def _():
                settle(i)

        @pl.when(t == per_block)
        def _():
            @pl.when(chosen)
            def _():
                z_cot[0].wait_recv()
                x_peer[0].start()
                core_peer[0].start()

            @pl.when(other)
            def _():
                x_own[0].wait_recv()
                core_relay[0].start()

        load_rows(t).wait()
        part[q, :, lanes(sub * CHUNK, CHUNK)] = rows_product(t)

        for i in range(5):
            @pl.when(t == 2 + i)
            def _():
                exchange(i).start()

        @pl.when(t == per_block)
        def _():
            core_part[0].start()

        @pl.when(t == T_AT)
        def _():
            send_tokens(0).start()

    load_rows(n_early).start()
    load_cols(0).start()
    core_part[0].wait_recv()

    @pl.loop(0, per_block)
    def _(k):
        at = lanes(k * CHUNK, CHUNK)
        part[1, :, at] = part[1, :, at] + crecv[0, :, at]

    best = maxima[5]
    step = jnp.maximum(best[0:8] * best[8:16] * (4.0 * rows / TOP), 1e-36)
    scales[0] = step
    scales[1] = 1.0 / step

    @pl.when(chosen)
    def _():
        z_cot[1].wait_recv()
        x_peer[1].start()
        core_peer[1].start()

    @pl.when(other)
    def _():
        x_own[1].wait_recv()
        core_relay[1].start()

    for s in range(1, AHEAD):
        send_tokens(s).start()

    def turn(dst, p):
        for r in range(2):
            j = z if r == 0 else 3 - z
            dst[r, :, :rows] = cotf[:, lanes(j * block + piece(p), half)].T
            dst[r, :, rows:] = cotp[r, :, lanes(piece(p), half)].T

    core_own.wait_recv()

    @pl.when(chosen)
    def _():
        core_relay[0].wait_recv()

    @pl.when(other)
    def _():
        x_peer[0].wait_recv()
        core_peer[0].start()

    core_peer[0].wait_recv()
    turn(cot_peer, 0)


    @pl.loop(0, n + Z_LAG)
    def _(s):
        @pl.when(s + AHEAD < n)
        def _():
            send_tokens(s + AHEAD).start()

        @pl.when(s == 1)
        def _():
            @pl.when(chosen)
            def _():
                core_relay[1].wait_recv()

            @pl.when(other)
            def _():
                x_peer[1].wait_recv()
                core_peer[1].start()

            core_peer[1].wait_recv()
            turn(cot_own, 1)

            @pl.when(other)
            def _():
                x_own[0].start()
                x_own[1].start()

        @pl.when(jnp.logical_and(s >= 1, s <= n))
        def _():
            k = s - 1
            send_y(k, 1).wait_recv()

            @pl.when(k >= SLOTS)
            def _():
                send_mirror(k - SLOTS).wait_send()

            total = product(cot_own.at[1], k) + decode(yrecv[k, 1], scales[0, 0:1, 0:1])
            msend[k % SLOTS] = encode(total, scales[1, 0:1, 0:1])
            wgrad[:, lanes(k * CHUNK, CHUNK)] = product(cot_own.at[0], k)
            send_mirror(k).start()

        @pl.when(s < n)
        def _():
            send_tokens(s).wait_recv()

            @pl.when(s >= SLOTS)
            def _():
                send_y(s - SLOTS, 0).wait_send()
                send_y(s - SLOTS, 1).wait_send()

            ysend[s % SLOTS, 1] = encode(product(cot_peer.at[1], s), scales[1, 0:1, 0:1])

            ysend[s % SLOTS, 0] = encode(product(cot_peer.at[0], s), scales[1, 0:1, 0:1])
            send_y(s, 1).start()

        @pl.when(s >= Z_LAG)
        def _():
            k = s - Z_LAG

            send_y(k, 0).wait_recv()
            at = lanes(k * CHUNK, CHUNK)
            wgrad[:, at] = wgrad[:, at] + decode(yrecv[k, 0], scales[0, 0:1, 0:1])

        @pl.when(s == 2)
        def _():
            x_part.start()

        @pl.when(s == HG_LAG)
        def _():
            for p in range(2):
                @pl.when(chosen)
                def _():
                    x_own[p].wait_recv()
                    core_relay[p].start()

            for p in range(2):
                @pl.when(other)
                def _():
                    core_relay[p].wait_recv()

        @pl.when(jnp.logical_and(s >= HG_LAG, s < n + HG_LAG))
        def _():
            t = s - HG_LAG

            @pl.when(t + 1 < n)
            def _():
                load_cols(t + 1).start()

            load_cols(t).wait()

            hgrad[:, lanes(t * CHUNK, CHUNK)] = jnp.dot(
                cotf[...], wcols[t % 2], preferred_element_type=f32
            ).astype(jnp.bfloat16)

        @pl.when(s < n)
        def _():
            send_y(s, 0).start()

        @pl.when(jnp.logical_and(s >= OUT_LAG, s < OUT_LAG + per_block))
        def _():
            t = n_early + s - OUT_LAG
            load_rows(t + 1).start()
            load_rows(t).wait()
            part[2, :, lanes((s - OUT_LAG) * CHUNK, CHUNK)] = rows_product(t)

        @pl.when(s == OUT_LAG + per_block)
        def _():
            core_part[1].start()

        @pl.when(s == OUT_END)
        def _():
            core_part[1].wait_recv()
            x_part.wait_recv()

        @pl.when(jnp.logical_and(s >= OUT_END, s < OUT_END + per_block))
        def _():
            k = s - OUT_END
            t = n_early + per_block + k

            @pl.when(k + 1 < per_block)
            def _():
                load_rows(t + 1).start()

            load_rows(t).wait()
            at = lanes(k * CHUNK, CHUNK)
            total = rows_product(t) + crecv[1, :, at] + xrecv[:, at]
            out[:, at] = total.astype(jnp.bfloat16)

        @pl.when(s >= Z_LAG)
        def _():
            k = s - Z_LAG
            send_mirror(k).wait_recv()
            at = lanes(k * CHUNK, CHUNK)
            wgrad[:, at] = (wgrad[:, at] + decode(mrecv[k], scales[0, 0:1, 0:1])) * grad_scale

    for k in range(SLOTS):
        send_y(n - SLOTS + k, 0).wait_send()
        send_y(n - SLOTS + k, 1).wait_send()
        send_mirror(n - SLOTS + k).wait_send()

    @pl.loop(0, n)
    def _(s):
        send_tokens(s).wait_send()

    for i in range(5):
        exchange(i).wait_send()
    core_own.wait_send()
    core_part[0].wait_send()
    core_part[1].wait_send()
    x_part.wait_send()
    for p in range(2):
        x_own[p].wait_send()
        core_relay[p].wait_send()
        core_peer[p].wait_send()

        @pl.when(chosen)
        def _():
            x_peer[p].wait_send()

        @pl.when(other)
        def _():
            z_cot[p].wait_send()


def shards_mirror(hidden, weight, cotangent):
    rows, width = hidden.shape
    block = cotangent.shape[1]
    features = weight.shape[0]
    n = width // CHUNK
    f32, bf16 = jnp.float32, jnp.bfloat16
    grad_scale = float(rows * lax.axis_size("gx")) ** (-0.5)
    dma = pltpu.SemaphoreType.DMA
    return pl.pallas_call(
        functools.partial(mirror_kernel, grad_scale),
        out_shape=(
            pltpu.VMEM((rows, block), bf16),
            pltpu.VMEM((rows, width), bf16),
            pltpu.VMEM((block // 2, width), f32),
        ),
        in_specs=[pl.BlockSpec(memory_space=pl.ANY)] * 3,
        out_specs=[pl.BlockSpec(memory_space=pltpu.VMEM)] * 3,
        scratch_shapes=[
            pltpu.VMEM((rows, width), bf16),
            pltpu.VMEM((n, rows, CHUNK), bf16),
            pltpu.VMEM((rows, features), bf16),
            pltpu.VMEM((2, rows, block), bf16),
            pltpu.VMEM((2, block // 2, 2 * rows), bf16),
            pltpu.VMEM((2, block // 2, 2 * rows), bf16),
            pltpu.VMEM((2, CHUNK, width), bf16),
            pltpu.VMEM((2, features, CHUNK), bf16),
            pltpu.VMEM((3, rows, block), f32),
            pltpu.VMEM((2, rows, block), f32),
            pltpu.VMEM((rows, block), f32),
            pltpu.VMEM((SLOTS, 2, block // 2, CHUNK), bf16),
            pltpu.VMEM((n, 2, block // 2, CHUNK), bf16),
            pltpu.VMEM((SLOTS, block // 2, CHUNK), bf16),
            pltpu.VMEM((n, block // 2, CHUNK), bf16),
            pltpu.VMEM((6, 16, LANES), f32),
            pltpu.VMEM((5, 16, LANES), f32),
            pltpu.VMEM((2, 8, LANES), f32),
            dma((2,)), dma((2,)), dma((2,)), dma((7,)), dma((7,)), dma((7,)), dma((7,)),
            dma((n,)), dma((n,)), dma((n, 2)), dma((n, 2)), dma((n,)), dma((n,)), dma((5,)),
            dma((5,)),
        ],
        compiler_params=pltpu.CompilerParams(
            collective_id=0, has_side_effects=True, vmem_limit_bytes=54_900_000
        ),
        name="mirror",
    )(hidden, weight, cotangent)


def solution(mesh):
    shape = dict(mesh.shape)
    mirror = shape["gx"] == 8 and shape["gy"] == 4
    return jax.shard_map(
        shards_mirror if mirror else shards_ring,
        mesh=mesh,
        in_specs=(P("gx", "gy"), P(None, "gy"), P("gx", "gy")),
        out_specs=(P("gx", "gy"), P("gx", "gy"), P("gx", "gy")),
        check_vma=False,
    )
```
